32 devices in a mesh: grp: 2 (over core), dev: 16 (over z, y, x).
Axes of the slice: x: 2, y: 2, z: 4, core: 2. Of those that a mesh axis runs over, the one named last changes fastest.
Arguments:
- emb_table: float32 [16384, 512], P(('grp', 'dev')), may hold values from -1.5 to 1.5
- adagrad_state: float32 [16384], P(('grp', 'dev')), may hold values from 0.05 to 1
- send_rows: int32 [32, 32, 32], P(('grp', 'dev')), may hold values from 0 to 511, as said below
- lookup_slot: int32 [8192, 8], P(('grp', 'dev')), may hold values from 0 to 1023, as said below
- seq_lengths: int32 [32, 2], P(('grp', 'dev')), may hold values from 0 to 256, as said below
- in_weight: bfloat16 [512, 2048], replicated, may hold values from -0.25 to 0.25
- out_weight: bfloat16 [512, 512], replicated, may hold values from -0.25 to 0.25
- norm_gain: float32 [512], replicated, may hold values from 0.5 to 1.5
- out_grad: bfloat16 [8192, 512], P(('grp', 'dev')), may hold values from -3 to 3
Outputs:
- layer_out: bfloat16 [8192, 512], P(('grp', 'dev'))
- table_new: float32 [16384, 512], P(('grp', 'dev'))
- state_new: float32 [16384], P(('grp', 'dev'))
- grad_in_weight: float32 [512, 2048], replicated
- grad_out_weight: float32 [512, 512], replicated
- grad_norm_gain: float32 [512], replicated
The draws below stay inside these ranges and needn't reach their ends.
Inputs may be any that keep to these rules, and one draw needn't show every extreme that they name: For each table shard o and device d, the 32 entries of send_rows[o, d] are distinct rows of the shard; every row of a shard is listed for exactly two different devices. `lookup_slot`: each device reads every one of its 1024 received rows at least once. `seq_lengths`: the 2 lengths of each device sum to 256; the first is at least 64, and a length of 0 means an empty slot, so a device holds one or two sequences.
All inputs are finite; a program needn't handle non-finite values.
Results may differ from the reference program's by a relative error of at most 0.012.
Values may be sent and summed in bfloat16 or wider, within the bound.
A program may use at most 64 MiB of HBM per device.

```python
import math
from functools import partial
import jax
import jax.numpy as jnp
from jax import lax

D = 512
HEADS = 4
FEATS = 8
TOK_DEV = 256
TOKENS = 8192
CAP = 32
RECV = 1024
ROWS_DEV = 512
NROWS = 16384
DEVICES = 32


def draw_send_rows(key, part):

    def one_shard(shard_key):
        first_key, second_key, order_key = jax.random.split(shard_key, 3)
        first_pass = jax.random.permutation(first_key, ROWS_DEV)
        second_pass = jax.random.permutation(second_key, ROWS_DEV)
        row_lists = jnp.concatenate([first_pass, second_pass]).reshape(DEVICES, CAP)
        dest_order = jax.random.permutation(order_key, DEVICES)
        return row_lists[dest_order]
    shard_keys = jax.random.split(jax.random.fold_in(key, 11), DEVICES)
    return jax.vmap(one_shard)(shard_keys).astype(jnp.int32)


def draw_lookup_slot(key, part):

    def one_device(device_key):
        cover_key, extra_key, shuffle_key = jax.random.split(device_key, 3)
        covered = jax.random.permutation(cover_key, RECV).astype(jnp.int32)
        extra_slots = jax.random.randint(extra_key, (TOK_DEV * FEATS - RECV,), 0, RECV).astype(jnp.int32)
        joined = jnp.concatenate([covered, extra_slots])
        return jax.random.permutation(shuffle_key, joined).reshape(TOK_DEV, FEATS)
    device_keys = jax.random.split(jax.random.fold_in(key, 23), DEVICES)
    return jax.vmap(one_device)(device_keys).reshape(TOKENS, FEATS).astype(jnp.int32)


def draw_seq_lengths(key, part):
    first_len = jax.random.randint(jax.random.fold_in(key, 37), (DEVICES, 1), TOK_DEV // 4, TOK_DEV + 1)
    first_len = first_len.astype(jnp.int32)
    second_len = (TOK_DEV - first_len).astype(jnp.int32)
    return jnp.concatenate([first_len, second_len], axis=1).astype(jnp.int32)


def block_scale(own_key, extent, cuts, least, top_value):
    level = 1.0
    for dim, shards_of in cuts:
        heights = jax.random.uniform(jax.random.fold_in(jax.random.fold_in(own_key, 6), dim), (shards_of,), jnp.float32, least / len(cuts), top_value / len(cuts))
        level = level * jnp.repeat(jnp.exp(heights), extent[dim] // shards_of).reshape((-1,) + (1,) * (len(extent) - 1 - dim))
    return level


def bell_draw(key, dims, deviation, most, shards=(), kind=jnp.bfloat16):
    entries = deviation * jax.random.normal(key, dims, jnp.float32)
    if shards:
        entries = entries * block_scale(key, dims, shards, -0.22, 0.18)
    return jnp.clip(entries, -most, most).astype(kind)


def setup_inputs(seed: int = 0) -> dict:
    streams_of = jax.random.split(jax.random.key(seed), 10)
    return {
        "emb_table": bell_draw(streams_of[0], (NROWS, D), 0.25, 1.5, ((0, 32),), jnp.float32),
        "adagrad_state": jnp.clip(jnp.exp(math.log(1.0) - 2.9957323 * jax.random.uniform(streams_of[1], (NROWS,), jnp.float32) ** block_scale(streams_of[1], (NROWS,), ((0, 32),), -0.2, 0.2)), 0.05, 1.0),
        "send_rows": draw_send_rows(jax.random.fold_in(streams_of[9], 71), 0),
        "lookup_slot": draw_lookup_slot(jax.random.fold_in(streams_of[9], 71), 0),
        "seq_lengths": draw_seq_lengths(jax.random.fold_in(streams_of[9], 71), 0),
        "in_weight": bell_draw(streams_of[5], (D, 4 * D), D ** -0.5, 0.25),
        "out_weight": bell_draw(streams_of[6], (D, D), D ** -0.5, 0.25),
        "norm_gain": jnp.clip(1.0 + 0.1 * jax.random.normal(streams_of[7], (D,), jnp.float32), 0.5, 1.5),
        "out_grad": bell_draw(streams_of[8], (TOKENS, D), 0.5, 3.0, ((0, 32),)),
    }


learn_rate = 0.2
norm_eps = 1e-05
adagrad_eps = 1e-08

def widened(pattern, left_op, right_op):
    return jnp.einsum(pattern, left_op.astype(jnp.float32), right_op.astype(jnp.float32))

def build_mask(lengths, slot_total):
    positions = jnp.arange(slot_total, dtype=jnp.int32)
    bounds = jnp.cumsum(lengths.astype(jnp.int32), dtype=jnp.int32).astype(jnp.int32)
    sequence_id = lax.optimization_barrier(jnp.sum((positions[:, None] >= bounds[None, :]).astype(jnp.int32), axis=1, dtype=jnp.int32))
    same_seq = sequence_id[:, None] == sequence_id[None, :]
    causal = positions[None, :] <= positions[:, None]
    return (same_seq & causal).astype(jnp.float32)

def attend(preact, norm_gain, seq_mask, head_count, product):
    activated = jax.nn.silu(preact).astype(jnp.bfloat16)
    tokens_here, stacked = activated.shape
    model_width = stacked // 4
    head_dim = model_width // head_count
    gate_part = activated[:, :model_width]
    values = activated[:, model_width:2 * model_width].reshape(tokens_here, head_count, head_dim)
    queries = activated[:, 2 * model_width:3 * model_width].reshape(tokens_here, head_count, head_dim)
    keys_all = activated[:, 3 * model_width:].reshape(tokens_here, head_count, head_dim)
    scores = product('thd,shd->hts', queries, keys_all) * (1.0 / math.sqrt(head_dim))
    weights = (jax.nn.silu(scores) * seq_mask).astype(jnp.bfloat16)
    attended = product('hts,shd->thd', weights, values).reshape(tokens_here, model_width)
    center = attended - lax.optimization_barrier(jnp.mean(attended, axis=1, keepdims=True))
    spread = lax.optimization_barrier(jnp.mean(center * center, axis=1, keepdims=True))
    normed = center * lax.rsqrt(spread + norm_eps)
    return (normed * norm_gain * gate_part.astype(jnp.float32)).astype(jnp.bfloat16)

def pool_rows(received, token_slots):
    pooled_sum = jnp.zeros((token_slots.shape[0], received.shape[1]), jnp.float32)
    for feature in range(token_slots.shape[1]):
        pooled_sum = pooled_sum + received[token_slots[:, feature]].astype(jnp.float32)
    return pooled_sum.astype(jnp.bfloat16)

def presum(d_pooled, token_slots, slot_total):
    spread = jnp.broadcast_to(d_pooled[:, None, :], (token_slots.shape[0], token_slots.shape[1], d_pooled.shape[1]))
    return jax.ops.segment_sum(spread.reshape(-1, d_pooled.shape[1]), token_slots.reshape(-1).astype(jnp.int32), num_segments=slot_total)

def dense_step(pooled, in_weight, out_weight, norm_gain, out_grad, seq_mask, head_count, product):
    preact = jnp.dot(pooled, in_weight, preferred_element_type=jnp.float32)
    mixed_out, pullback = jax.vjp(partial(attend, seq_mask=seq_mask, head_count=head_count, product=product), preact, norm_gain)
    layer_out = (jnp.dot(mixed_out, out_weight, preferred_element_type=jnp.float32) + pooled.astype(jnp.float32)).astype(jnp.bfloat16)
    grad_wout = jnp.dot(mixed_out.T, out_grad, preferred_element_type=jnp.float32)
    d_mixed = jnp.dot(out_grad, out_weight.T, preferred_element_type=jnp.float32).astype(jnp.bfloat16)
    d_preact, d_gain = pullback(d_mixed)
    d_low = d_preact.astype(jnp.bfloat16)
    grad_win = jnp.dot(pooled.T, d_low, preferred_element_type=jnp.float32)
    d_pooled = jnp.dot(d_low, in_weight.T, preferred_element_type=jnp.float32) + out_grad.astype(jnp.float32)
    return (layer_out, grad_win, grad_wout, d_gain.astype(jnp.float32), d_pooled)

def reference(emb_table, adagrad_state, send_rows, lookup_slot, seq_lengths, in_weight, out_weight, norm_gain, out_grad):
    send_rows = send_rows.astype(jnp.int32)
    lookup_slot = lookup_slot.astype(jnp.int32)
    seq_lengths = seq_lengths.astype(jnp.int32)
    owners = jnp.arange(DEVICES, dtype=jnp.int32)

    def one_device(running, device_index):
        grad_table, sum_win, sum_wout, sum_gain = running
        picked = lax.dynamic_index_in_dim(send_rows, device_index, 1, keepdims=False).astype(jnp.int32)
        global_rows = (owners[:, None] * ROWS_DEV + picked).reshape(-1).astype(jnp.int32)
        received = emb_table[global_rows].astype(jnp.bfloat16)
        start = (device_index * TOK_DEV).astype(jnp.int32)
        token_slots = lax.dynamic_slice_in_dim(lookup_slot, start, TOK_DEV, 0).astype(jnp.int32)
        cotangent = lax.dynamic_slice_in_dim(out_grad, start, TOK_DEV, 0)
        lengths = lax.dynamic_index_in_dim(seq_lengths, device_index, 0, keepdims=False).astype(jnp.int32)
        pooled = pool_rows(received, token_slots)
        seq_mask = build_mask(lengths, TOK_DEV)
        layer_out, grad_win, grad_wout, d_gain, d_pooled = dense_step(pooled, in_weight, out_weight, norm_gain, cotangent, seq_mask, HEADS, widened)
        row_grad = presum(d_pooled, token_slots, RECV).astype(jnp.float32)
        grad_table = grad_table.at[global_rows].add(row_grad)
        return ((grad_table, sum_win + grad_win.astype(jnp.float32), sum_wout + grad_wout.astype(jnp.float32), sum_gain + d_gain), layer_out)
    initial = (jnp.zeros((NROWS, D), jnp.float32), jnp.zeros((D, 4 * D), jnp.float32), jnp.zeros((D, D), jnp.float32), jnp.zeros((D,), jnp.float32))
    finals, out_blocks = lax.scan(one_device, initial, jnp.arange(DEVICES, dtype=jnp.int32))
    grad_rows, sum_win, sum_wout, sum_gain = finals
    grad_scale = 1.0 / math.sqrt(TOKENS)
    state_new = adagrad_state + lax.optimization_barrier(jnp.mean(grad_rows * grad_rows, axis=1))
    table_new = emb_table - learn_rate * grad_rows / (jnp.sqrt(state_new)[:, None] + adagrad_eps)
    return (out_blocks.reshape(TOKENS, D), table_new, state_new, sum_win * grad_scale, sum_wout * grad_scale, sum_gain * grad_scale)
```

```python
from functools import partial
import math

import jax
import jax.numpy as jnp
from jax import lax
from jax.experimental import pallas as pl
from jax.experimental.pallas import tpu as pltpu
from jax.sharding import PartitionSpec as P

HEADS = 4
FAN = 4
ROWS_FIRST = True
ROTATE_NUM, ROTATE_DEN = 1, 4


learn_rate = 0.2
norm_eps = 1e-05
adagrad_eps = 1e-08


def narrow(pattern, left_op, right_op):
    return jnp.einsum(pattern, left_op, right_op, preferred_element_type=jnp.float32)


def build_mask(lengths, slot_total):
    positions = jnp.arange(slot_total, dtype=jnp.int32)
    bounds = jnp.cumsum(lengths, dtype=jnp.int32)
    sequence_id = jnp.sum(
        (positions[:, None] >= bounds[None, :]).astype(jnp.int32), axis=1, dtype=jnp.int32
    )
    same_seq = sequence_id[:, None] == sequence_id[None, :]
    causal = positions[None, :] <= positions[:, None]
    return (same_seq & causal).astype(jnp.float32)


def attend(preact, norm_gain, seq_mask, head_count, product):
    activated = jax.nn.silu(preact).astype(jnp.bfloat16)
    tokens_here, stacked = activated.shape
    model_width = stacked // 4
    head_dim = model_width // head_count
    gate_part = activated[:, :model_width]
    values = activated[:, model_width : 2 * model_width].reshape(tokens_here, head_count, head_dim)
    queries = activated[:, 2 * model_width : 3 * model_width].reshape(
        tokens_here, head_count, head_dim
    )
    keys_all = activated[:, 3 * model_width :].reshape(tokens_here, head_count, head_dim)
    scores = product("thd,shd->hts", queries, keys_all) * (1.0 / math.sqrt(head_dim))
    weights = (jax.nn.silu(scores) * seq_mask).astype(jnp.bfloat16)
    attended = product("hts,shd->thd", weights, values).reshape(tokens_here, model_width)
    center = attended - jnp.mean(attended, axis=1, keepdims=True)
    spread = jnp.mean(center * center, axis=1, keepdims=True)
    normed = center * lax.rsqrt(spread + norm_eps)
    return (normed * norm_gain * gate_part.astype(jnp.float32)).astype(jnp.bfloat16)


def count_matrix(token_slots, slot_total):
    slots = jnp.arange(slot_total, dtype=jnp.int32)
    counts = jnp.zeros((token_slots.shape[0], slot_total), jnp.float32)
    for feature in range(token_slots.shape[1]):
        counts = counts + (token_slots[:, feature : feature + 1] == slots[None, :]).astype(
            jnp.float32
        )
    return counts.astype(jnp.bfloat16)


def row_picker(row_lists, row_total):
    rows = jnp.arange(row_total, dtype=jnp.int32)
    return (row_lists.reshape(-1, 1) == rows[None, :]).astype(jnp.bfloat16)


def dense_step(pooled, in_weight, out_weight, norm_gain, out_grad, seq_mask, head_count, product):
    preact = jnp.dot(pooled, in_weight, preferred_element_type=jnp.float32)
    mixed_out, pullback = jax.vjp(
        partial(attend, seq_mask=seq_mask, head_count=head_count, product=product),
        preact,
        norm_gain,
    )
    layer_out = (
        jnp.dot(mixed_out, out_weight, preferred_element_type=jnp.float32)
        + pooled.astype(jnp.float32)
    ).astype(jnp.bfloat16)
    grad_wout = jnp.dot(mixed_out.T, out_grad, preferred_element_type=jnp.float32)
    d_mixed = jnp.dot(out_grad, out_weight.T, preferred_element_type=jnp.float32).astype(
        jnp.bfloat16
    )
    d_preact, d_gain = pullback(d_mixed)
    d_low = d_preact.astype(jnp.bfloat16)
    grad_win = jnp.dot(pooled.T, d_low, preferred_element_type=jnp.float32)
    d_pooled = jnp.dot(d_low, in_weight.T, preferred_element_type=jnp.float32) + out_grad.astype(
        jnp.float32
    )
    return (layer_out, grad_win, grad_wout, d_gain, d_pooled)


def exchange_kernel(
    peers,
    dev_count,
    levels,
    row_ref,
    gain_ref,
    grad_ref,
    arrive_ref,
    gain_out,
    full_ref,
    *scratch,
):
    half_in, half_sum = scratch[0], scratch[1]
    level_in = scratch[2 : 2 + levels]
    level_sum = scratch[2 + levels : 2 + 2 * levels]
    gains, row_send, row_recv, gain_send, gain_recv, tree_send, tree_recv = scratch[
        2 + 2 * levels :
    ]
    grp = lax.axis_index("grp")
    dev = lax.axis_index("dev")
    me = grp * dev_count + dev
    other = 1 - grp
    barrier = pltpu.get_barrier_semaphore()

    def place(step):
        target = lax.rem(me + step, peers)
        return (target // dev_count, lax.rem(target, dev_count))

    def greet(step, carry):
        pl.semaphore_signal(
            barrier, inc=1, device_id=place(step), device_id_type=pl.DeviceIdType.MESH
        )
        return carry

    lax.fori_loop(1, peers, greet, 0)
    pl.semaphore_wait(barrier, peers - 1)

    def tree_copy(index, source, landing, target):
        return pltpu.make_async_remote_copy(
            src_ref=source,
            dst_ref=landing,
            send_sem=tree_send.at[index],
            recv_sem=tree_recv.at[index],
            device_id=target,
            device_id_type=pl.DeviceIdType.MESH,
        )

    half = peers // 2
    first = tree_copy(0, grad_ref.at[pl.ds(other * half, half)], half_in, (other, dev))
    first.start()

    def row_copy(step):
        target = lax.rem(me + step, peers)
        return pltpu.make_async_remote_copy(
            src_ref=row_ref.at[target],
            dst_ref=arrive_ref.at[me],
            send_sem=row_send.at[step],
            recv_sem=row_recv.at[step],
            device_id=place(step),
            device_id_type=pl.DeviceIdType.MESH,
        )

    def row_landing(step):
        source = lax.rem(me + peers - step, peers)
        return pltpu.make_async_remote_copy(
            src_ref=row_ref.at[source],
            dst_ref=arrive_ref.at[source],
            send_sem=row_send.at[step],
            recv_sem=row_recv.at[step],
            device_id=place(step),
            device_id_type=pl.DeviceIdType.MESH,
        )

    def gain_copy(step):
        return pltpu.make_async_remote_copy(
            src_ref=gain_ref,
            dst_ref=gains.at[step],
            send_sem=gain_send.at[step],
            recv_sem=gain_recv.at[step],
            device_id=place(step),
            device_id_type=pl.DeviceIdType.MESH,
        )

    def launch(i, carry):
        step = 1 + lax.rem(i + ROTATE_NUM * peers // ROTATE_DEN, peers - 1)
        row_copy(step).start()
        gain_copy(step).start()
        return carry

    if ROWS_FIRST:
        lax.fori_loop(0, peers - 1, launch, 0)
    arrive_ref[me] = row_ref[me]
    gains[0] = gain_ref[...]
    first.wait()

    def add_half(i, carry):
        half_sum[i] = (
            grad_ref[grp * half + i].astype(jnp.float32) + half_in[i].astype(jnp.float32)
        ).astype(jnp.bfloat16)
        return carry

    lax.fori_loop(0, half, add_half, 0)
    held, span, stride, slot = half_sum, half, 1, 1
    base = grp * half
    bases = []
    for level in range(levels):
        digit = lax.rem(dev // stride, FAN)
        part = span // FAN
        copies = []
        for step in range(1, FAN):
            there = lax.rem(digit + step, FAN)
            target = (grp, dev + (there - digit) * stride)
            copies.append(
                tree_copy(
                    slot, held.at[pl.ds(there * part, part)], level_in[level].at[step - 1], target
                )
            )
            copies[-1].start()
            slot += 1
        if level == 0 and not ROWS_FIRST:
            lax.fori_loop(0, peers - 1, launch, 0)
        for copy in copies:
            copy.wait()
        final = level == levels - 1
        base = base + digit * part

        def add_level(i, carry, held=held, level=level, digit=digit, part=part, final=final, base=base):
            total = held[digit * part + i].astype(jnp.float32)
            for step in range(FAN - 1):
                total = total + level_in[level][step, i].astype(jnp.float32)
            if final:
                full_ref[base + i] = total.astype(jnp.bfloat16)
            else:
                level_sum[level][i] = total.astype(jnp.bfloat16)
            return carry

        lax.fori_loop(0, part, add_level, 0)
        bases.append((base, part, digit, stride))
        held, span, stride = level_sum[level], part, stride * FAN
    for base, part, digit, stride in reversed(bases):
        copies = []
        for step in range(1, FAN):
            there = lax.rem(digit + step, FAN)
            target = (grp, dev + (there - digit) * stride)
            block = full_ref.at[pl.ds(base, part)]
            copies.append((slot, step, tree_copy(slot, block, block, target)))
            copies[-1][2].start()
            slot += 1
        for index, step, copy in copies:
            copy.wait_send()
            source = lax.rem(digit + FAN - step, FAN)
            block = full_ref.at[pl.ds(base + (source - digit) * part, part)]
            tree_copy(index, block, block, (grp, dev)).wait_recv()
    mine = full_ref.at[pl.ds(grp * half, half)]
    theirs = full_ref.at[pl.ds(other * half, half)]
    last = tree_copy(slot, mine, mine, (other, dev))
    last.start()

    def finish(step, carry):
        row_copy(step).wait_send()
        row_landing(step).wait_recv()
        gain_copy(step).wait()
        return carry

    lax.fori_loop(1, peers, finish, 0)
    gain_out[...] = jnp.sum(gains[...], axis=0)
    last.wait_send()
    tree_copy(slot, theirs, theirs, (other, dev)).wait_recv()


def exchange(row_grad, gain, grads):
    peers, chunk, width = grads.shape
    dev_count = lax.axis_size("dev")
    levels, reach = 0, 1
    while reach < dev_count:
        levels, reach = levels + 1, reach * FAN
    if reach != dev_count or peers != 2 * dev_count:
        raise ValueError("unsupported mesh")
    spans = [peers // 2 // FAN ** (k + 1) for k in range(levels)]
    copies = 2 + 2 * (FAN - 1) * levels
    low = jnp.bfloat16
    vmem = pl.BlockSpec(memory_space=pltpu.VMEM)
    return pl.pallas_call(
        partial(exchange_kernel, peers, dev_count, levels),
        out_shape=(
            jax.ShapeDtypeStruct(row_grad.shape, row_grad.dtype),
            jax.ShapeDtypeStruct(gain.shape, gain.dtype),
            jax.ShapeDtypeStruct(grads.shape, grads.dtype),
        ),
        in_specs=[vmem] * 3,
        out_specs=(vmem,) * 3,
        scratch_shapes=[
            pltpu.VMEM((peers // 2, chunk, width), low),
            pltpu.VMEM((peers // 2, chunk, width), low),
            *[pltpu.VMEM((FAN - 1, span, chunk, width), low) for span in spans],
            *[pltpu.VMEM((span, chunk, width), low) for span in spans],
            pltpu.VMEM((peers,) + gain.shape, jnp.float32),
            pltpu.SemaphoreType.DMA((peers,)),
            pltpu.SemaphoreType.DMA((peers,)),
            pltpu.SemaphoreType.DMA((peers,)),
            pltpu.SemaphoreType.DMA((peers,)),
            pltpu.SemaphoreType.DMA((copies,)),
            pltpu.SemaphoreType.DMA((copies,)),
        ],
        compiler_params=pltpu.CompilerParams(
            collective_id=0, has_side_effects=True, vmem_limit_bytes=40 * 1024 * 1024
        ),
        name="exchange",
    )(row_grad, gain, grads)


def body(
    emb_table,
    adagrad_state,
    send_rows,
    lookup_slot,
    seq_lengths,
    in_weight,
    out_weight,
    norm_gain,
    out_grad,
):
    row_lists = send_rows[0]
    peer_count, slot_count = row_lists.shape
    row_width = emb_table.shape[1]
    picker = row_picker(row_lists, emb_table.shape[0])
    outgoing = jnp.dot(
        picker, emb_table.astype(jnp.bfloat16), preferred_element_type=jnp.float32
    ).astype(jnp.bfloat16)
    outgoing = outgoing.reshape(peer_count, slot_count, row_width)
    incoming = lax.all_to_all(outgoing, ("grp", "dev"), split_axis=0, concat_axis=0, tiled=True)
    received = incoming.reshape(peer_count * slot_count, row_width)
    counts = count_matrix(lookup_slot, peer_count * slot_count)
    pooled = jnp.dot(counts, received, preferred_element_type=jnp.float32).astype(jnp.bfloat16)
    seq_mask = build_mask(seq_lengths[0], lookup_slot.shape[0])
    layer_out, grad_win, grad_wout, d_gain, d_pooled = dense_step(
        pooled, in_weight, out_weight, norm_gain, out_grad, seq_mask, HEADS, narrow
    )
    row_grad = lax.dot_general(
        counts,
        d_pooled.astype(jnp.bfloat16),
        (((0,), (0,)), ((), ())),
        preferred_element_type=jnp.float32,
    ).astype(jnp.bfloat16)
    stacked = jnp.concatenate(
        [part.astype(jnp.bfloat16) for part in jnp.split(grad_win, 4, axis=1) + [grad_wout]]
    )
    arriving, gain_sum, grad_sums = exchange(
        row_grad.reshape(peer_count, slot_count, row_width),
        d_gain[None, :],
        stacked.reshape(peer_count, -1, row_width),
    )
    grad_blocks = grad_sums.reshape(5, row_width, row_width)
    grad_rows = lax.dot_general(
        picker,
        arriving.reshape(peer_count * slot_count, row_width),
        (((0,), (0,)), ((), ())),
        preferred_element_type=jnp.float32,
    )
    state_new = adagrad_state + jnp.mean(grad_rows * grad_rows, axis=1)
    table_new = emb_table - learn_rate * grad_rows / (jnp.sqrt(state_new)[:, None] + adagrad_eps)
    grad_scale = 1.0 / math.sqrt(lookup_slot.shape[0] * peer_count)
    return (
        layer_out,
        table_new,
        state_new,
        jnp.concatenate([grad_blocks[k].astype(jnp.float32) * grad_scale for k in range(4)], axis=1),
        grad_blocks[4].astype(jnp.float32) * grad_scale,
        gain_sum[0] * grad_scale,
    )


def solution(mesh):
    in_specs = (
        P(("grp", "dev"), None),
        P(("grp", "dev")),
        P(("grp", "dev"), None, None),
        P(("grp", "dev"), None),
        P(("grp", "dev"), None),
        P(),
        P(),
        P(),
        P(("grp", "dev"), None),
    )
    out_specs = (P(("grp", "dev"), None), P(("grp", "dev"), None), P(("grp", "dev")), P(), P(), P())
    return jax.shard_map(body, mesh=mesh, in_specs=in_specs, out_specs=out_specs, check_vma=False)
```

```python
from functools import partial
import math

import jax
import jax.numpy as jnp
from jax import lax
from jax.experimental import pallas as pl
from jax.experimental.pallas import tpu as pltpu
from jax.sharding import PartitionSpec as P

HEADS = 4
FAN = 4
ROWS_FIRST = True
ROTATE_NUM, ROTATE_DEN = 1, 4


learn_rate = 0.2
norm_eps = 1e-05
adagrad_eps = 1e-08


def build_mask(lengths, slot_total):
    positions = jnp.arange(slot_total, dtype=jnp.int32)
    bounds = jnp.cumsum(lengths, dtype=jnp.int32)
    sequence_id = jnp.sum(
        (positions[:, None] >= bounds[None, :]).astype(jnp.int32), axis=1, dtype=jnp.int32
    )
    same_seq = sequence_id[:, None] == sequence_id[None, :]
    causal = positions[None, :] <= positions[:, None]
    return (same_seq & causal).astype(jnp.float32)


def count_matrix(token_slots, slot_total):
    slots = jnp.arange(slot_total, dtype=jnp.int32)
    counts = jnp.zeros((token_slots.shape[0], slot_total), jnp.float32)
    for feature in range(token_slots.shape[1]):
        counts = counts + (token_slots[:, feature : feature + 1] == slots[None, :]).astype(
            jnp.float32
        )
    return counts.astype(jnp.bfloat16)


def spread_matrix(token_slots, slot_total):
    slots = jnp.arange(slot_total, dtype=jnp.int32)
    across = token_slots.T
    counts = jnp.zeros((slot_total, token_slots.shape[0]), jnp.float32)
    for feature in range(token_slots.shape[1]):
        counts = counts + (slots[:, None] == across[feature : feature + 1]).astype(jnp.float32)
    return counts.astype(jnp.bfloat16)


def row_picker(row_lists, row_total):
    rows = jnp.arange(row_total, dtype=jnp.int32)
    return (row_lists.reshape(-1, 1) == rows[None, :]).astype(jnp.bfloat16)


def mul(left_op, right_op, left_dim, right_dim):
    return lax.dot_general(
        left_op,
        right_op,
        (((left_dim,), (right_dim,)), ((), ())),
        preferred_element_type=jnp.float32,
    )


def layer_kernel(
    counts_ref,
    spread_ref,
    received_ref,
    win_ref,
    wout_ref,
    gain_ref,
    cot_ref,
    dmixed_ref,
    mask_ref,
    layer_ref,
    grads_ref,
    dgain_ref,
    row_ref,
    slope_ref,
    low_ref,
):
    low = jnp.bfloat16
    width = cot_ref.shape[1]
    head_dim = width // HEADS
    scale = 1.0 / math.sqrt(head_dim)
    pooled = mul(counts_ref[...], received_ref[...], 1, 0).astype(low)
    active = []
    for block in range(4):
        columns = pl.ds(block * width, width)
        preact = mul(pooled, win_ref[:, columns], 1, 0)
        gate = jax.nn.sigmoid(preact)
        active.append((preact * gate).astype(low))
        slope_ref[:, columns] = gate * (1.0 + preact * (1.0 - gate))
    gate_part, values, queries, keys_all = active
    gate_part = gate_part.astype(jnp.float32)
    mask = mask_ref[...]
    weights, slopes, parts = [], [], []
    for head in range(HEADS):
        cut = slice(head * head_dim, (head + 1) * head_dim)
        scores = mul(queries[:, cut], keys_all[:, cut], 1, 1) * scale
        gate = jax.nn.sigmoid(scores)
        weights.append((scores * gate * mask).astype(low))
        slopes.append(gate * (1.0 + scores * (1.0 - gate)) * mask)
        parts.append(mul(weights[-1], values[:, cut], 1, 0))
    attended = jnp.concatenate(parts, axis=1)
    center = attended - jnp.mean(attended, axis=1, keepdims=True)
    spread = jnp.mean(center * center, axis=1, keepdims=True)
    inverse = lax.rsqrt(spread + norm_eps)
    normed = center * inverse
    gain = gain_ref[...]
    mixed = (normed * gain * gate_part).astype(low)
    layer_ref[...] = (mul(mixed, wout_ref[...], 1, 0) + pooled.astype(jnp.float32)).astype(low)
    grads_ref[pl.ds(4 * width, width), :] = mul(mixed, cot_ref[...], 0, 0).astype(low)
    d_mixed = dmixed_ref[...].astype(jnp.float32)
    dgain_ref[...] = jnp.sum(d_mixed * normed * gate_part, axis=0, keepdims=True)
    d_gate = (d_mixed * (normed * gain)).astype(low)
    low_ref[:, pl.ds(0, width)] = (
        d_gate.astype(jnp.float32) * slope_ref[:, pl.ds(0, width)]
    ).astype(low)
    d_normed = d_mixed * gate_part * gain
    d_attended = inverse * (
        d_normed
        - jnp.mean(d_normed, axis=1, keepdims=True)
        - normed * jnp.mean(d_normed * normed, axis=1, keepdims=True)
    )
    d_attended = d_attended.astype(low)
    for head in range(HEADS):
        cut = slice(head * head_dim, (head + 1) * head_dim)
        d_part = d_attended[:, cut]
        d_weights = mul(d_part, values[:, cut], 1, 1).astype(low)
        d_scores = (d_weights.astype(jnp.float32) * slopes[head] * scale).astype(low)
        for block, grad in (
            (1, mul(weights[head], d_part, 0, 0)),
            (2, mul(d_scores, keys_all[:, cut], 1, 0)),
            (3, mul(d_scores, queries[:, cut], 0, 0)),
        ):
            columns = pl.ds(block * width + head * head_dim, head_dim)
            low_ref[:, columns] = (
                grad.astype(low).astype(jnp.float32) * slope_ref[:, columns]
            ).astype(low)
    d_low = low_ref[...]
    d_pooled = mul(d_low, win_ref[...], 1, 1) + cot_ref[...].astype(jnp.float32)
    row_ref[...] = mul(spread_ref[...], d_pooled.astype(low), 1, 0).astype(low)
    grad_win = mul(pooled, d_low, 0, 0).astype(low)
    for block in range(4):
        grads_ref[pl.ds(block * width, width), :] = grad_win[:, block * width : (block + 1) * width]


def layer(counts, spread, received, in_weight, out_weight, norm_gain, out_grad, d_mixed, seq_mask):
    tokens, width = out_grad.shape
    low = jnp.bfloat16
    vmem = pl.BlockSpec(memory_space=pltpu.VMEM)
    return pl.pallas_call(
        layer_kernel,
        out_shape=(
            jax.ShapeDtypeStruct((tokens, width), low),
            jax.ShapeDtypeStruct((5 * width, width), low),
            jax.ShapeDtypeStruct((1, width), jnp.float32),
            jax.ShapeDtypeStruct((spread.shape[0], width), low),
        ),
        in_specs=[vmem] * 9,
        out_specs=(vmem,) * 4,
        scratch_shapes=[
            pltpu.VMEM((tokens, 4 * width), jnp.float32),
            pltpu.VMEM((tokens, 4 * width), low),
        ],
        cost_estimate=pl.CostEstimate(
            flops=26 * tokens * width * width, bytes_accessed=1 << 23, transcendentals=1 << 20
        ),
        compiler_params=pltpu.CompilerParams(vmem_limit_bytes=40 * 1024 * 1024),
        name="layer",
    )(counts, spread, received, in_weight, out_weight, norm_gain, out_grad, d_mixed, seq_mask)


def exchange_kernel(
    peers,
    dev_count,
    levels,
    row_ref,
    gain_ref,
    grad_ref,
    arrive_ref,
    gain_out,
    full_ref,
    *scratch,
):
    half_in, half_sum = scratch[0], scratch[1]
    level_in = scratch[2 : 2 + levels]
    level_sum = scratch[2 + levels : 2 + 2 * levels]
    gains, row_send, row_recv, gain_send, gain_recv, tree_send, tree_recv = scratch[
        2 + 2 * levels :
    ]
    grp = lax.axis_index("grp")
    dev = lax.axis_index("dev")
    me = grp * dev_count + dev
    other = 1 - grp
    barrier = pltpu.get_barrier_semaphore()

    def place(step):
        target = lax.rem(me + step, peers)
        return (target // dev_count, lax.rem(target, dev_count))

    def greet(step, carry):
        pl.semaphore_signal(
            barrier, inc=1, device_id=place(step), device_id_type=pl.DeviceIdType.MESH
        )
        return carry

    lax.fori_loop(1, peers, greet, 0)
    pl.semaphore_wait(barrier, peers - 1)

    def tree_copy(index, source, landing, target):
        return pltpu.make_async_remote_copy(
            src_ref=source,
            dst_ref=landing,
            send_sem=tree_send.at[index],
            recv_sem=tree_recv.at[index],
            device_id=target,
            device_id_type=pl.DeviceIdType.MESH,
        )

    half = peers // 2
    first = tree_copy(0, grad_ref.at[pl.ds(other * half, half)], half_in, (other, dev))
    first.start()

    def row_copy(step):
        target = lax.rem(me + step, peers)
        return pltpu.make_async_remote_copy(
            src_ref=row_ref.at[target],
            dst_ref=arrive_ref.at[me],
            send_sem=row_send.at[step],
            recv_sem=row_recv.at[step],
            device_id=place(step),
            device_id_type=pl.DeviceIdType.MESH,
        )

    def row_landing(step):
        source = lax.rem(me + peers - step, peers)
        return pltpu.make_async_remote_copy(
            src_ref=row_ref.at[source],
            dst_ref=arrive_ref.at[source],
            send_sem=row_send.at[step],
            recv_sem=row_recv.at[step],
            device_id=place(step),
            device_id_type=pl.DeviceIdType.MESH,
        )

    def gain_copy(step):
        return pltpu.make_async_remote_copy(
            src_ref=gain_ref,
            dst_ref=gains.at[step],
            send_sem=gain_send.at[step],
            recv_sem=gain_recv.at[step],
            device_id=place(step),
            device_id_type=pl.DeviceIdType.MESH,
        )

    def launch(i, carry):
        step = 1 + lax.rem(i + ROTATE_NUM * peers // ROTATE_DEN, peers - 1)
        row_copy(step).start()
        gain_copy(step).start()
        return carry

    if ROWS_FIRST:
        lax.fori_loop(0, peers - 1, launch, 0)
    arrive_ref[me] = row_ref[me]
    gains[0] = gain_ref[...]
    first.wait()

    def add_half(i, carry):
        half_sum[i] = (
            grad_ref[grp * half + i].astype(jnp.float32) + half_in[i].astype(jnp.float32)
        ).astype(jnp.bfloat16)
        return carry

    lax.fori_loop(0, half, add_half, 0)
    held, span, stride, slot = half_sum, half, 1, 1
    base = grp * half
    bases = []
    for level in range(levels):
        digit = lax.rem(dev // stride, FAN)
        part = span // FAN
        copies = []
        for step in range(1, FAN):
            there = lax.rem(digit + step, FAN)
            target = (grp, dev + (there - digit) * stride)
            copies.append(
                tree_copy(
                    slot, held.at[pl.ds(there * part, part)], level_in[level].at[step - 1], target
                )
            )
            copies[-1].start()
            slot += 1
        if level == 0 and not ROWS_FIRST:
            lax.fori_loop(0, peers - 1, launch, 0)
        for copy in copies:
            copy.wait()
        final = level == levels - 1
        base = base + digit * part

        def add_level(i, carry, held=held, level=level, digit=digit, part=part, final=final, base=base):
            total = held[digit * part + i].astype(jnp.float32)
            for step in range(FAN - 1):
                total = total + level_in[level][step, i].astype(jnp.float32)
            if final:
                full_ref[base + i] = total.astype(jnp.bfloat16)
            else:
                level_sum[level][i] = total.astype(jnp.bfloat16)
            return carry

        lax.fori_loop(0, part, add_level, 0)
        bases.append((base, part, digit, stride))
        held, span, stride = level_sum[level], part, stride * FAN
    for base, part, digit, stride in reversed(bases):
        copies = []
        for step in range(1, FAN):
            there = lax.rem(digit + step, FAN)
            target = (grp, dev + (there - digit) * stride)
            block = full_ref.at[pl.ds(base, part)]
            copies.append((slot, step, tree_copy(slot, block, block, target)))
            copies[-1][2].start()
            slot += 1
        for index, step, copy in copies:
            copy.wait_send()
            source = lax.rem(digit + FAN - step, FAN)
            block = full_ref.at[pl.ds(base + (source - digit) * part, part)]
            tree_copy(index, block, block, (grp, dev)).wait_recv()
    mine = full_ref.at[pl.ds(grp * half, half)]
    theirs = full_ref.at[pl.ds(other * half, half)]
    last = tree_copy(slot, mine, mine, (other, dev))
    last.start()

    def finish(step, carry):
        row_copy(step).wait_send()
        row_landing(step).wait_recv()
        gain_copy(step).wait()
        return carry

    lax.fori_loop(1, peers, finish, 0)
    gain_out[...] = jnp.sum(gains[...], axis=0)
    last.wait_send()
    tree_copy(slot, theirs, theirs, (other, dev)).wait_recv()


def exchange(row_grad, gain, grads):
    peers, chunk, width = grads.shape
    dev_count = lax.axis_size("dev")
    levels, reach = 0, 1
    while reach < dev_count:
        levels, reach = levels + 1, reach * FAN
    if reach != dev_count or peers != 2 * dev_count:
        raise ValueError("unsupported mesh")
    spans = [peers // 2 // FAN ** (k + 1) for k in range(levels)]
    copies = 2 + 2 * (FAN - 1) * levels
    low = jnp.bfloat16
    vmem = pl.BlockSpec(memory_space=pltpu.VMEM)
    return pl.pallas_call(
        partial(exchange_kernel, peers, dev_count, levels),
        out_shape=(
            jax.ShapeDtypeStruct(row_grad.shape, row_grad.dtype),
            jax.ShapeDtypeStruct(gain.shape, gain.dtype),
            jax.ShapeDtypeStruct(grads.shape, grads.dtype),
        ),
        in_specs=[vmem] * 3,
        out_specs=(vmem,) * 3,
        scratch_shapes=[
            pltpu.VMEM((peers // 2, chunk, width), low),
            pltpu.VMEM((peers // 2, chunk, width), low),
            *[pltpu.VMEM((FAN - 1, span, chunk, width), low) for span in spans],
            *[pltpu.VMEM((span, chunk, width), low) for span in spans],
            pltpu.VMEM((peers,) + gain.shape, jnp.float32),
            pltpu.SemaphoreType.DMA((peers,)),
            pltpu.SemaphoreType.DMA((peers,)),
            pltpu.SemaphoreType.DMA((peers,)),
            pltpu.SemaphoreType.DMA((peers,)),
            pltpu.SemaphoreType.DMA((copies,)),
            pltpu.SemaphoreType.DMA((copies,)),
        ],
        compiler_params=pltpu.CompilerParams(
            collective_id=0, has_side_effects=True, vmem_limit_bytes=40 * 1024 * 1024
        ),
        name="exchange",
    )(row_grad, gain, grads)


def body(
    emb_table,
    adagrad_state,
    send_rows,
    lookup_slot,
    seq_lengths,
    in_weight,
    out_weight,
    norm_gain,
    out_grad,
):
    row_lists = send_rows[0]
    peer_count, slot_count = row_lists.shape
    row_width = emb_table.shape[1]
    picker = row_picker(row_lists, emb_table.shape[0])
    outgoing = jnp.dot(
        picker, emb_table.astype(jnp.bfloat16), preferred_element_type=jnp.float32
    ).astype(jnp.bfloat16)
    outgoing = outgoing.reshape(peer_count, slot_count, row_width)
    incoming = lax.all_to_all(outgoing, ("grp", "dev"), split_axis=0, concat_axis=0, tiled=True)
    received = incoming.reshape(peer_count * slot_count, row_width)
    counts = count_matrix(lookup_slot, peer_count * slot_count)
    spread = spread_matrix(lookup_slot, peer_count * slot_count)
    seq_mask = build_mask(seq_lengths[0], lookup_slot.shape[0])
    d_mixed = jnp.dot(out_grad, out_weight.T, preferred_element_type=jnp.float32).astype(
        jnp.bfloat16
    )
    layer_out, grads, d_gain, row_grad = layer(
        counts,
        spread,
        received,
        in_weight,
        out_weight,
        norm_gain[None, :],
        out_grad,
        d_mixed,
        seq_mask,
    )
    arriving, gain_sum, grad_sums = exchange(
        row_grad.reshape(peer_count, slot_count, row_width),
        d_gain,
        grads.reshape(peer_count, -1, row_width),
    )
    grad_blocks = grad_sums.reshape(5, row_width, row_width)
    grad_rows = lax.dot_general(
        picker,
        arriving.reshape(peer_count * slot_count, row_width),
        (((0,), (0,)), ((), ())),
        preferred_element_type=jnp.float32,
    )
    state_new = adagrad_state + jnp.mean(grad_rows * grad_rows, axis=1)
    table_new = emb_table - learn_rate * grad_rows / (jnp.sqrt(state_new)[:, None] + adagrad_eps)
    grad_scale = 1.0 / math.sqrt(lookup_slot.shape[0] * peer_count)
    return (
        layer_out,
        table_new,
        state_new,
        jnp.concatenate([grad_blocks[k].astype(jnp.float32) * grad_scale for k in range(4)], axis=1),
        grad_blocks[4].astype(jnp.float32) * grad_scale,
        gain_sum[0] * grad_scale,
    )


def solution(mesh):
    in_specs = (
        P(("grp", "dev"), None),
        P(("grp", "dev")),
        P(("grp", "dev"), None, None),
        P(("grp", "dev"), None),
        P(("grp", "dev"), None),
        P(),
        P(),
        P(),
        P(("grp", "dev"), None),
    )
    out_specs = (P(("grp", "dev"), None), P(("grp", "dev"), None), P(("grp", "dev")), P(), P(), P())
    return jax.shard_map(body, mesh=mesh, in_specs=in_specs, out_specs=out_specs, check_vma=False)
```
